32 devices in a mesh: iface: 8 (over z, y), dom: 4 (over x, core).
Axes of the slice: x: 2, y: 2, z: 4, core: 2. Of those that a mesh axis runs over, the one named last changes fastest.
Arguments:
- interface: float32 [131072], P(('iface', 'dom')), may hold values from -6 to 6
- previous_residual: float32 [131072], P(('iface', 'dom')), may hold values from -6 to 6
- previous_estimate: float32 [131072], P(('iface', 'dom')), may hold values from -6 to 6
- forcing: float32 [131072], P(('iface', 'dom')), may hold values from -60 to 60
- stiffness: float32 [131072], P(('iface', 'dom')), may hold values from 0.2 to 0.6
- history_residual: float32 [100, 131072], P(None, ('iface', 'dom')), may hold values from -40 to 40
- history_estimate: float32 [100, 131072], P(None, ('iface', 'dom')), may hold values from -6 to 6
Outputs:
- interface_next: float32 [131072], P(('iface', 'dom'))
- residual_last: float32 [131072], P(('iface', 'dom'))
The draws below stay inside these ranges and needn't reach their ends.
All inputs are finite; a program needn't handle non-finite values.
Results may differ from the reference program's by a relative error of at most 0.0003.
Values sent between devices are 32-bit elements; how exact they have to be, the bound alone decides.
A program may use at most 64 MiB of HBM per device.

```python
import math
import jax
import jax.numpy as jnp
from jax import lax

HIST = 100
ITERS = 3
NI = 131072


def shared_history(key):
    high = lax.Precision.HIGHEST
    base = jax.random.normal(jax.random.fold_in(key, 7), (HIST + 1, NI), jnp.float32)
    factors = jax.random.uniform(jax.random.fold_in(key, 11), (HIST, 1), jnp.float32, 0.4, 0.8)
    banded = base[1:] + factors * base[:-1]
    mixing = jnp.eye(HIST, dtype=jnp.float32) + 0.2 * jax.random.normal(jax.random.fold_in(key, 12), (HIST, HIST), jnp.float32) / math.sqrt(HIST)
    mixed = jnp.dot(mixing, banded, precision=high)
    return jnp.clip(mixed, -40.0, 40.0)


def draw_history_residual(key, part):
    return shared_history(key)


def draw_forcing(key, part):
    mixed = shared_history(key)
    weights = jax.random.normal(jax.random.fold_in(key, 9), (HIST,), jnp.float32) / math.sqrt(HIST)
    noise = jax.random.normal(jax.random.fold_in(key, 10), (NI,), jnp.float32)
    total = 0.8 * jnp.dot(weights, mixed, precision=lax.Precision.HIGHEST) + 0.5 * noise
    return jnp.clip(total, -60.0, 60.0)


def shard_levels(key, shape, pieces, least, high):
    level = 1.0
    for axis_at, shards_of in pieces:
        steps = jax.random.uniform(jax.random.fold_in(jax.random.fold_in(key, 6), axis_at), (shards_of,), jnp.float32, least / len(pieces), high / len(pieces))
        level = level * jnp.repeat(jnp.exp(steps), shape[axis_at] // shards_of).reshape((-1,) + (1,) * (len(shape) - 1 - axis_at))
    return level


def normal_values(rng, shape, deviation, most, shards=(), kind=jnp.bfloat16):
    loudness = shard_levels(rng, shape, shards, -0.22, 0.18) if shards else 1.0
    drawn = jax.random.normal(rng, shape, jnp.float32) * deviation * loudness
    return jnp.minimum(jnp.maximum(drawn, -most), most).astype(kind)


def setup_inputs(seed: int = 0) -> dict:
    streams_of = jax.random.split(jax.random.key(seed), 8)
    interface = normal_values(streams_of[0], (NI,), 1.0, 6.0, ((0, 32),), jnp.float32)
    previous_residual = normal_values(streams_of[1], (NI,), 1.0, 6.0, ((0, 32),), jnp.float32)
    previous_estimate = normal_values(streams_of[2], (NI,), 1.0, 6.0, ((0, 32),), jnp.float32)
    forcing = draw_forcing(jax.random.fold_in(streams_of[7], 71), 0)
    stiffness = jnp.clip(0.2 + 0.400000021 * jax.random.uniform(streams_of[4], (NI,), jnp.float32) ** shard_levels(streams_of[4], (NI,), ((0, 32),), -0.2, 0.2), 0.2, 0.6)
    history_residual = draw_history_residual(jax.random.fold_in(streams_of[7], 71), 0)
    history_estimate = normal_values(streams_of[6], (HIST, NI), 1.0, 6.0, ((1, 32),), jnp.float32)
    return dict(interface=interface, previous_residual=previous_residual, previous_estimate=previous_estimate, forcing=forcing, stiffness=stiffness, history_residual=history_residual, history_estimate=history_estimate)


coupling = 0.25

def solver_map(current, forcing, stiffness):
    padded = jnp.pad(current, 1)
    return forcing + stiffness * jnp.tanh(current) + coupling * (padded[:-2] + padded[2:])

def reference(interface, previous_residual, previous_estimate, forcing, stiffness, history_residual, history_estimate):
    high = lax.Precision.HIGHEST
    current = interface
    hist_v = history_residual
    hist_w = history_estimate
    old_residual = previous_residual
    old_estimate = previous_estimate
    residual = previous_residual
    for iteration in range(ITERS):
        estimate = solver_map(current, forcing, stiffness)
        residual = estimate - current
        hist_v = jnp.concatenate([hist_v, (residual - old_residual)[None, :]], axis=0)
        hist_w = jnp.concatenate([hist_w, (estimate - old_estimate)[None, :]], axis=0)
        gram_matrix = jnp.dot(hist_v, hist_v.T, precision=high)
        projection = jnp.dot(hist_v, residual, precision=high)
        factor = jnp.linalg.cholesky(gram_matrix)
        coeffs = -jax.scipy.linalg.cho_solve((factor, True), projection)
        current = estimate + jnp.dot(coeffs, hist_w, precision=high)
        old_residual = residual
        old_estimate = estimate
    return (current, residual)
```

```python
import functools
import jax
import jax.numpy as jnp
from jax import lax
from jax.experimental import pallas as pl
from jax.experimental.pallas import tpu as pltpu
from jax.sharding import PartitionSpec as P

ITERS = 3
coupling = 0.25
LANES = 128
AXES = ("iface", "dom")
F32 = jnp.float32


def invert(matrix, rows):
    lane8 = lax.broadcasted_iota(jnp.int32, (8, LANES), 1)
    sub8 = lax.broadcasted_iota(jnp.int32, (8, LANES), 0)
    blocks = [matrix[8 * at : 8 * at + 8, :] for at in range(rows // 8)]
    for step in range(rows // 8):
        first = 8 * step
        inside = (lane8 >= first) & (lane8 < first + 8)
        unit = (lane8 - first == sub8).astype(F32)
        pivots = blocks[step]
        columns = [jnp.broadcast_to(pivots[:, first + at : first + at + 1], (8, LANES)) for at in range(8)]
        panel = jnp.where(inside, unit, pivots)
        for at in range(8):
            inverse = 1.0 / columns[at][at : at + 1, :]
            own = sub8 == at
            factor = columns[at]
            row = panel[at : at + 1, :] * inverse
            panel = jnp.where(own, row, panel - factor * row)
            for later in range(at + 1, 8):
                row = columns[later][at : at + 1, :] * inverse
                columns[later] = jnp.where(own, row, columns[later] - factor * row)
        for other in range(rows // 8):
            if other != step:
                block = blocks[other]
                total = jnp.where(inside, 0.0, block)
                for at in range(8):
                    column = jnp.broadcast_to(block[:, first + at : first + at + 1], (8, LANES))
                    total = total - column * panel[at : at + 1, :]
                blocks[other] = total
        blocks[step] = panel
    return jnp.concatenate(blocks, axis=0)


def kernel(
    sizes,
    interface,
    previous_residual,
    previous_estimate,
    forcing,
    stiffness,
    history_residual,
    history_estimate,
    next_ref,
    last_ref,
    cur_x,
    est_x,
    force_x,
    stiff_x,
    old_res,
    hist_v,
    hist_w,
    new_v,
    new_w,
    dots_in,
    square,
    part_out,
    part_in,
    gathered,
    row_in,
    load_sem,
    halo_sem,
    wide_sem,
    part_sem,
    gather_sem,
    row_sem,
):
    n_iface, n_dom, hist, base, rows, width, share = sizes
    count = n_iface * n_dom
    me = lax.axis_index("iface") * n_dom + lax.axis_index("dom")
    full = width + 2 * LANES

    def place(index):
        return (index // n_dom, lax.rem(index, n_dom))

    def peer(step):
        return lax.rem(me + step, count)

    barrier = pltpu.get_barrier_semaphore()

    @pl.loop(1, count)
    def _(step):
        pl.semaphore_signal(barrier, inc=1, device_id=place(peer(step)), device_id_type=pl.DeviceIdType.MESH)

    own = pl.ds(LANES, width)
    load_v = pltpu.make_async_copy(history_residual, hist_v, load_sem.at[0])
    load_v.start()
    small = []
    for at, (source, target) in enumerate(
        [
            (interface, cur_x.at[:, own]),
            (previous_estimate, est_x.at[:, own]),
            (forcing, force_x.at[:, own]),
            (stiffness, stiff_x.at[:, own]),
            (previous_residual, old_res),
        ]
    ):
        copy = pltpu.make_async_copy(source, target, load_sem.at[2 + at])
        copy.start()
        small.append(copy)
    load_w = pltpu.make_async_copy(history_estimate, hist_w.at[:, own], load_sem.at[1])
    load_w.start()
    new_v[...] = jnp.zeros(new_v.shape, F32)
    new_w[...] = jnp.zeros(new_w.shape, F32)

    load_v.wait()
    depth = 512

    def add_gram(at, total):
        block = hist_v[:, pl.ds(pl.multiple_of(at * depth, depth), depth)]
        return total + lax.dot_general(
            block, block, (((1,), (1,)), ((), ())), precision=lax.Precision.HIGHEST, preferred_element_type=F32
        )

    gram = lax.fori_loop(0, width // depth, add_gram, jnp.zeros((hist, hist), F32))
    square[...] = jnp.zeros(square.shape, F32)
    square[0:hist, 0:hist] = gram
    for at in range(count):
        part_out[at] = square[at * share : (at + 1) * share, :]
    part_in[me] = part_out[me]
    for copy in small:
        copy.wait()
    load_w.wait()
    pl.semaphore_wait(barrier, count - 1)

    halos = []
    right, left = place(peer(1)), place(peer(count - 1))
    for at, ref in enumerate([cur_x, est_x, force_x, stiff_x]):
        for side, (source, target, device) in enumerate([(width, 0, right), (LANES, width + LANES, left)]):
            copy = pltpu.make_async_remote_copy(
                src_ref=ref.at[:, pl.ds(source, LANES)],
                dst_ref=ref.at[:, pl.ds(target, LANES)],
                send_sem=halo_sem.at[0, at, side],
                recv_sem=halo_sem.at[1, at, side],
                device_id=device,
                device_id_type=pl.DeviceIdType.MESH,
            )
            copy.start()
            halos.append(copy)

    def exchange(source_of, target, sems):
        def send(step):
            to = peer(step)
            return pltpu.make_async_remote_copy(
                src_ref=source_of(to),
                dst_ref=target.at[me],
                send_sem=sems.at[0],
                recv_sem=sems.at[1],
                device_id=place(to),
                device_id_type=pl.DeviceIdType.MESH,
            )

        @pl.loop(1, count)
        def _(step):
            send(step).start()

    def arrive(target, sems):
        most = target.at[pl.ds(0, count - 1)]
        pltpu.make_async_copy(most, most, sems.at[1]).wait()
        pltpu.make_async_copy(most, most, sems.at[0]).wait()

    exchange(lambda to: part_out.at[to], part_in, part_sem)
    wide = []
    for side, (source, target, device) in enumerate([(width, 0, right), (LANES, width + LANES, left)]):
        copy = pltpu.make_async_remote_copy(
            src_ref=hist_w.at[:, pl.ds(source, LANES)],
            dst_ref=hist_w.at[:, pl.ds(target, LANES)],
            send_sem=wide_sem.at[0, side],
            recv_sem=wide_sem.at[1, side],
            device_id=device,
            device_id_type=pl.DeviceIdType.MESH,
        )
        copy.start()
        wide.append(copy)
    for copy in halos:
        copy.wait()

    lane = lax.broadcasted_iota(jnp.int32, (1, full), 1)
    outside = ((me == 0) & (lane < LANES)) | ((me == count - 1) & (lane >= LANES + width))
    eye = (
        lax.broadcasted_iota(jnp.int32, (rows, LANES), 0) == lax.broadcasted_iota(jnp.int32, (rows, LANES), 1)
    ).astype(F32)
    row_at = lax.broadcasted_iota(jnp.int32, (rows, LANES), 0)
    ones = jnp.ones((8, LANES), F32)
    cur_x[...] = jnp.where(outside, 0.0, cur_x[...])

    def column_of(row):
        return jnp.broadcast_to(jnp.sum(eye * row, axis=1, keepdims=True), (rows, LANES))

    def over_rows(value):
        return jnp.sum(value, axis=0, keepdims=True)

    def begin(iteration):
        current = cur_x[...]
        before = pltpu.roll(current, 1, 1)
        after = pltpu.roll(current, full - 1, 1)
        estimate = force_x[...] + stiff_x[...] * jnp.tanh(current) + coupling * (before + after)
        residual = (estimate - current)[:, LANES : LANES + width]
        new_w[iteration : iteration + 1, :] = estimate - est_x[...]
        est_x[...] = estimate
        new_v[iteration : iteration + 1, :] = residual - old_res[...]
        old_res[...] = residual

        def add(at, totals):
            span = pl.ds(pl.multiple_of(at * LANES, LANES), LANES)
            block, extra = hist_v[:, span], new_v[:, span]
            res, new = old_res[:, span], new_v[iteration : iteration + 1, span]
            return (totals[0] + block * res, totals[1] + block * new, totals[2] + extra * res, totals[3] + extra * new)

        zero, few = jnp.zeros((hist, LANES), F32), jnp.zeros((8, LANES), F32)
        totals = lax.fori_loop(0, width // LANES, add, (zero, zero, few, few), unroll=4)
        dots_in[iteration] = jnp.zeros((2, LANES), F32)
        for which in range(4):
            sums = lax.dot_general(
                ones, totals[which], (((1,), (1,)), ((), ())), precision=lax.Precision.HIGHEST, preferred_element_type=F32
            )
            if which < 2:
                dots_in[iteration, which : which + 1, 0:hist] = sums[0:1, :]
            else:
                dots_in[iteration, which - 2 : which - 1, base : base + 8] = sums[0:1, :]
        row_in[iteration, me] = dots_in[iteration]
        exchange(lambda to: dots_in.at[iteration], row_in.at[iteration], row_sem.at[iteration])

    def sums_of(iteration):
        arrive(row_in.at[iteration], row_sem.at[iteration])
        return jnp.sum(row_in[iteration], axis=0)

    begin(0)

    arrive(part_in, part_sem)
    gathered[me] = jnp.sum(part_in[...], axis=0)
    exchange(lambda to: gathered.at[me], gathered, gather_sem)
    arrive(gathered, gather_sem)
    for at in range(-(-base // share)):
        square[at * share : (at + 1) * share, :] = gathered[at]
    kept = (row_at < hist) & (lax.broadcasted_iota(jnp.int32, (rows, LANES), 1) < hist)
    square[0:rows, :] = jnp.where(kept, square[0:rows, :], eye)
    square[0:base, :] = invert(square, base)
    square[0:rows, :] = jnp.where(kept, square[0:rows, :], 0.0)
    for copy in wide:
        copy.wait()

    solved, columns = [], []
    for iteration in range(ITERS):
        both = sums_of(iteration)
        proj, new = both[0:1, :], both[1:2, :]
        inverse = square[0:rows, :]
        proj_col, new_col = column_of(proj), column_of(new)
        proj_sol = jnp.broadcast_to(jnp.sum(inverse * proj, axis=1, keepdims=True), (rows, LANES))
        new_sol = jnp.broadcast_to(jnp.sum(inverse * new, axis=1, keepdims=True), (rows, LANES))
        solved.append(new_sol)
        columns.append(new_col)
        size = iteration + 1
        schur = [
            [columns[a][base + b : base + b + 1, :] - over_rows(columns[a] * solved[b]) for b in range(a + 1)]
            for a in range(size)
        ]
        right_side = [proj_col[base + a : base + a + 1, :] - over_rows(columns[a] * proj_sol) for a in range(size)]
        for a in range(size):
            for b in range(a + 1, size):
                factor = schur[b][a] / schur[a][a]
                right_side[b] = right_side[b] - factor * right_side[a]
                for c in range(a + 1, b + 1):
                    schur[b][c] = schur[b][c] - factor * schur[c][a]
        answer = [None] * size
        for a in reversed(range(size)):
            value = right_side[a]
            for b in range(a + 1, size):
                value = value - schur[b][a] * answer[b]
            answer[a] = value / schur[a][a]
        weights = proj_sol
        for a in range(size):
            weights = jnp.where(row_at == base + a, answer[a], weights - solved[a] * answer[a])

        def combine(at, carry):
            span = pl.ds(pl.multiple_of(at * LANES, LANES), LANES)
            cur_x[:, span] = (
                est_x[:, span]
                - over_rows(hist_w[:, span] * weights[0:hist, :])
                - over_rows(new_w[:, span] * weights[base:rows, :])
            )
            return carry

        lax.fori_loop(0, full // LANES, combine, 0, unroll=2)
        if iteration + 1 < ITERS:
            cur_x[...] = jnp.where(outside, 0.0, cur_x[...])
            begin(iteration + 1)
    next_ref[...] = cur_x[:, LANES : LANES + width]
    last_ref[...] = old_res[...]


def shards(n_iface, n_dom, *args):
    width = args[0].shape[0]
    hist = args[5].shape[0]
    base = -(-hist // 8) * 8
    rows = base + 8
    count = n_iface * n_dom
    share = -(-base // count)
    full = width + 2 * LANES
    vectors = [a.reshape(1, width) for a in args[:5]]
    any_spec = pl.BlockSpec(memory_space=pl.ANY)
    vmem_spec = pl.BlockSpec(memory_space=pltpu.VMEM)
    outs = pl.pallas_call(
        functools.partial(kernel, (n_iface, n_dom, hist, base, rows, width, share)),
        out_shape=[jax.ShapeDtypeStruct((1, width), F32)] * 2,
        in_specs=[any_spec] * 7,
        out_specs=[vmem_spec] * 2,
        scratch_shapes=[
            pltpu.VMEM((1, full), F32),
            pltpu.VMEM((1, full), F32),
            pltpu.VMEM((1, full), F32),
            pltpu.VMEM((1, full), F32),
            pltpu.VMEM((1, width), F32),
            pltpu.VMEM((hist, width), F32),
            pltpu.VMEM((hist, full), F32),
            pltpu.VMEM((8, width), F32),
            pltpu.VMEM((8, full), F32),
            pltpu.VMEM((ITERS, 2, LANES), F32),
            pltpu.VMEM((max(LANES, share * count), LANES), F32),
            pltpu.VMEM((count, share, LANES), F32),
            pltpu.VMEM((count, share, LANES), F32),
            pltpu.VMEM((count, share, LANES), F32),
            pltpu.VMEM((ITERS, count, 2, LANES), F32),
            pltpu.SemaphoreType.DMA((7,)),
            pltpu.SemaphoreType.DMA((2, 4, 2)),
            pltpu.SemaphoreType.DMA((2, 2)),
            pltpu.SemaphoreType.DMA((2,)),
            pltpu.SemaphoreType.DMA((2,)),
            pltpu.SemaphoreType.DMA((ITERS, 2)),
        ],
        compiler_params=pltpu.CompilerParams(collective_id=0, has_side_effects=True),
        name="coupling",
    )(*vectors, args[5], args[6])
    return outs[0].reshape(width), outs[1].reshape(width)


def solution(mesh):
    one = P(AXES)
    return jax.shard_map(
        functools.partial(shards, mesh.shape["iface"], mesh.shape["dom"]),
        mesh=mesh,
        in_specs=(one,) * 5 + (P(None, AXES),) * 2,
        out_specs=(one, one),
        check_vma=False,
    )
```

```python
import functools
import jax
import jax.numpy as jnp
from jax import lax
from jax.experimental import pallas as pl
from jax.experimental.pallas import tpu as pltpu
from jax.sharding import PartitionSpec as P

ITERS = 3
coupling = 0.25
LANES = 128
AXES = ("iface", "dom")
F32 = jnp.float32


def invert(matrix, rows):
    lane8 = lax.broadcasted_iota(jnp.int32, (8, LANES), 1)
    sub8 = lax.broadcasted_iota(jnp.int32, (8, LANES), 0)
    blocks = [matrix[8 * at : 8 * at + 8, :] for at in range(rows // 8)]
    for step in range(rows // 8):
        first = 8 * step
        inside = (lane8 >= first) & (lane8 < first + 8)
        unit = (lane8 - first == sub8).astype(F32)
        pivots = blocks[step]
        columns = [jnp.broadcast_to(pivots[:, first + at : first + at + 1], (8, LANES)) for at in range(8)]
        panel = jnp.where(inside, unit, pivots)
        for at in range(8):
            inverse = 1.0 / columns[at][at : at + 1, :]
            own = sub8 == at
            factor = columns[at]
            row = panel[at : at + 1, :] * inverse
            panel = jnp.where(own, row, panel - factor * row)
            for later in range(at + 1, 8):
                row = columns[later][at : at + 1, :] * inverse
                columns[later] = jnp.where(own, row, columns[later] - factor * row)
        for other in range(rows // 8):
            if other != step:
                block = blocks[other]
                total = jnp.where(inside, 0.0, block)
                for at in range(8):
                    column = jnp.broadcast_to(block[:, first + at : first + at + 1], (8, LANES))
                    total = total - column * panel[at : at + 1, :]
                blocks[other] = total
        blocks[step] = panel
    return jnp.concatenate(blocks, axis=0)


def kernel(
    sizes,
    interface,
    previous_residual,
    previous_estimate,
    forcing,
    stiffness,
    history_residual,
    history_estimate,
    next_ref,
    last_ref,
    cur_x,
    est_x,
    force_x,
    stiff_x,
    old_res,
    hist_v,
    hist_w,
    new_v,
    new_w,
    dots_in,
    square,
    part_out,
    part_in,
    mid_in,
    gathered,
    row_in,
    piece_sem,
    load_sem,
    halo_sem,
    wide_sem,
    part_sem,
    mid_sem,
    gather_sem,
    row_sem,
):
    n_iface, n_dom, hist, base, rows, width, share, depth = sizes
    count = n_iface * n_dom
    at_iface, at_dom = lax.axis_index("iface"), lax.axis_index("dom")
    me = at_iface * n_dom + at_dom
    last = count - 1
    full = width + 2 * LANES
    ifaces = [lax.rem(at_iface + step, n_iface) for step in range(n_iface)]
    doms = [lax.rem(at_dom + step, n_dom) for step in range(n_dom)]
    everyone = [(a, b) for a in ifaces for b in doms][1:]

    def place(index):
        return (index // n_dom, lax.rem(index, n_dom))

    barrier = pltpu.get_barrier_semaphore()
    for device in everyone:
        pl.semaphore_signal(barrier, inc=1, device_id=device, device_id_type=pl.DeviceIdType.MESH)

    own = pl.ds(LANES, width)

    def piece(at):
        span = pl.ds(pl.multiple_of(at * depth, depth), depth)
        return pltpu.make_async_copy(history_residual.at[:, span], hist_v.at[:, span], piece_sem.at[at])

    for at in range(width // depth):
        piece(at).start()
    small = []
    for at, (source, target) in enumerate(
        [
            (interface, cur_x.at[:, own]),
            (previous_estimate, est_x.at[:, own]),
            (forcing, force_x.at[:, own]),
            (stiffness, stiff_x.at[:, own]),
            (previous_residual, old_res),
        ]
    ):
        copy = pltpu.make_async_copy(source, target, load_sem.at[1 + at])
        copy.start()
        small.append(copy)
    load_w = pltpu.make_async_copy(history_estimate, hist_w.at[:, own], load_sem.at[0])
    new_v[...] = jnp.zeros(new_v.shape, F32)
    new_w[...] = jnp.zeros(new_w.shape, F32)

    def add_gram(at, total):
        piece(at).wait()
        block = hist_v[:, pl.ds(pl.multiple_of(at * depth, depth), depth)]
        return total + lax.dot_general(
            block, block, (((1,), (1,)), ((), ())), precision=lax.Precision.HIGHEST, preferred_element_type=F32
        )

    gram = lax.fori_loop(0, width // depth, add_gram, jnp.zeros((hist, hist), F32))
    load_w.start()
    square[...] = jnp.zeros(square.shape, F32)
    square[0:hist, 0:hist] = gram
    lane8 = lax.broadcasted_iota(jnp.int32, (8, LANES), 1)
    blocks = (base // 8 + 1) // 2 * 2
    pairs = blocks // 2

    def natural(block):
        return (lane8 >= 8 * block) & (lane8 < 8 * blocks)

    for pair in range(n_dom * share):
        where = (pair // share, pl.ds(8 * (pair % share), 8), slice(None))
        if pair < pairs:
            other = blocks - 1 - pair
            moved = pltpu.roll(square[8 * other : 8 * other + 8, :], 8 * pair + 8, 1)
            part_out[where] = jnp.where(natural(pair), square[8 * pair : 8 * pair + 8, :], moved)
        else:
            part_out[where] = jnp.zeros((8, LANES), F32)
    part_in[at_dom] = part_out[at_dom]
    for copy in small:
        copy.wait()
    pl.semaphore_wait(barrier, last)

    right = place(lax.rem(me + 1, count))
    left = place(lax.rem(me + last, count))

    def edges(refs, sems):
        copies = []
        for at, ref in enumerate(refs):
            for side, (source, target, device) in enumerate([(width, 0, right), (LANES, width + LANES, left)]):
                copies.append(
                    pltpu.make_async_remote_copy(
                        src_ref=ref.at[:, pl.ds(source, LANES)],
                        dst_ref=ref.at[:, pl.ds(target, LANES)],
                        send_sem=sems.at[0, at, side],
                        recv_sem=sems.at[1, at, side],
                        device_id=device,
                        device_id_type=pl.DeviceIdType.MESH,
                    )
                )
        return copies[0::2], copies[1::2]

    def edges_start(copies):
        for side, some in enumerate([me < last, me > 0]):

            @pl.when(some)
            def _():
                for copy in copies[side]:
                    copy.start()

    def edges_wait(copies):
        for side, (sent, received) in enumerate([(me < last, me > 0), (me > 0, me < last)]):

            @pl.when(sent)
            def _():
                for copy in copies[side]:
                    copy.wait_send()

            @pl.when(received)
            def _():
                for copy in copies[side]:
                    copy.wait_recv()

    def send(source, target, sems, device):
        pltpu.make_async_remote_copy(
            src_ref=source,
            dst_ref=target,
            send_sem=sems.at[0],
            recv_sem=sems.at[1],
            device_id=device,
            device_id_type=pl.DeviceIdType.MESH,
        ).start()

    def arrive(target, many, sems):
        most = target.at[pl.ds(0, many)]
        pltpu.make_async_copy(most, most, sems.at[1]).wait()
        pltpu.make_async_copy(most, most, sems.at[0]).wait()

    for dom in doms[1:]:
        send(part_out.at[dom], part_in.at[at_dom], part_sem, (at_iface, dom))
    halos = edges([cur_x, est_x, force_x, stiff_x], halo_sem)
    edges_start(halos)
    wide = edges([hist_w], wide_sem)

    lane = lax.broadcasted_iota(jnp.int32, (1, full), 1)
    outside = ((me == 0) & (lane < LANES)) | ((me == count - 1) & (lane >= LANES + width))
    eye = (
        lax.broadcasted_iota(jnp.int32, (rows, LANES), 0) == lax.broadcasted_iota(jnp.int32, (rows, LANES), 1)
    ).astype(F32)
    row_at = lax.broadcasted_iota(jnp.int32, (rows, LANES), 0)
    ones = jnp.ones((8, LANES), F32)

    def column_of(row):
        return jnp.broadcast_to(jnp.sum(eye * row, axis=1, keepdims=True), (rows, LANES))

    def over_rows(value):
        return jnp.sum(value, axis=0, keepdims=True)

    def begin(iteration):
        current = cur_x[...]
        before = pltpu.roll(current, 1, 1)
        after = pltpu.roll(current, full - 1, 1)
        estimate = force_x[...] + stiff_x[...] * jnp.tanh(current) + coupling * (before + after)
        residual = (estimate - current)[:, LANES : LANES + width]
        new_w[iteration : iteration + 1, :] = estimate - est_x[...]
        est_x[...] = estimate
        new_v[iteration : iteration + 1, :] = residual - old_res[...]
        old_res[...] = residual

        def add(at, totals):
            span = pl.ds(pl.multiple_of(at * LANES, LANES), LANES)
            block, extra = hist_v[:, span], new_v[:, span]
            res, new = old_res[:, span], new_v[iteration : iteration + 1, span]
            return (totals[0] + block * res, totals[1] + block * new, totals[2] + extra * res, totals[3] + extra * new)

        zero, few = jnp.zeros((hist, LANES), F32), jnp.zeros((8, LANES), F32)
        totals = lax.fori_loop(0, width // LANES, add, (zero, zero, few, few), unroll=4)
        dots_in[iteration] = jnp.zeros((2, LANES), F32)
        for which in range(4):
            sums = lax.dot_general(
                ones, totals[which], (((1,), (1,)), ((), ())), precision=lax.Precision.HIGHEST, preferred_element_type=F32
            )
            if which < 2:
                dots_in[iteration, which : which + 1, 0:hist] = sums[0:1, :]
            else:
                dots_in[iteration, which - 2 : which - 1, base : base + 8] = sums[0:1, :]
        row_in[iteration, me] = dots_in[iteration]
        for device in everyone:
            send(dots_in.at[iteration], row_in.at[iteration, me], row_sem.at[iteration], device)

    def sums_of(iteration):
        arrive(row_in.at[iteration], last, row_sem.at[iteration])
        return jnp.sum(row_in[iteration], axis=0)

    arrive(part_in, n_dom - 1, part_sem)
    mid_in[at_iface] = jnp.sum(part_in[...], axis=0)
    for iface in ifaces[1:]:
        send(mid_in.at[at_iface], mid_in.at[at_iface], mid_sem, (iface, at_dom))
    edges_wait(halos)
    cur_x[...] = jnp.where(outside, 0.0, cur_x[...])
    begin(0)
    load_w.wait()
    edges_start(wide)
    arrive(mid_in, n_iface - 1, mid_sem)
    gathered[at_dom] = jnp.sum(mid_in[...], axis=0)
    for dom in doms[1:]:
        send(gathered.at[at_dom], gathered.at[at_dom], gather_sem, (at_iface, dom))
    arrive(gathered, n_dom - 1, gather_sem)
    for pair in range(pairs):
        other = blocks - 1 - pair
        packed = gathered[pair // share, pl.ds(8 * (pair % share), 8), :]
        square[8 * pair : 8 * pair + 8, :] = jnp.where(natural(pair), packed, 0.0)
        moved = pltpu.roll(packed, LANES - 8 * pair - 8, 1)
        square[8 * other : 8 * other + 8, :] = jnp.where(natural(other), moved, 0.0)
    upper = square[...]
    lane_block = lax.broadcasted_iota(jnp.int32, (LANES, LANES), 1) // 8
    row_block = lax.broadcasted_iota(jnp.int32, (LANES, LANES), 0) // 8
    square[...] = jnp.where(lane_block >= row_block, upper, upper.T)
    kept = (row_at < hist) & (lax.broadcasted_iota(jnp.int32, (rows, LANES), 1) < hist)
    square[0:rows, :] = jnp.where(kept, square[0:rows, :], eye)
    square[0:base, :] = invert(square, base)
    square[0:rows, :] = jnp.where(kept, square[0:rows, :], 0.0)
    edges_wait(wide)

    solved, columns = [], []
    for iteration in range(ITERS):
        both = sums_of(iteration)
        proj, new = both[0:1, :], both[1:2, :]
        inverse = square[0:rows, :]
        proj_col, new_col = column_of(proj), column_of(new)
        proj_sol = jnp.broadcast_to(jnp.sum(inverse * proj, axis=1, keepdims=True), (rows, LANES))
        new_sol = jnp.broadcast_to(jnp.sum(inverse * new, axis=1, keepdims=True), (rows, LANES))
        solved.append(new_sol)
        columns.append(new_col)
        size = iteration + 1
        schur = [
            [columns[a][base + b : base + b + 1, :] - over_rows(columns[a] * solved[b]) for b in range(a + 1)]
            for a in range(size)
        ]
        right_side = [proj_col[base + a : base + a + 1, :] - over_rows(columns[a] * proj_sol) for a in range(size)]
        for a in range(size):
            for b in range(a + 1, size):
                factor = schur[b][a] / schur[a][a]
                right_side[b] = right_side[b] - factor * right_side[a]
                for c in range(a + 1, b + 1):
                    schur[b][c] = schur[b][c] - factor * schur[c][a]
        answer = [None] * size
        for a in reversed(range(size)):
            value = right_side[a]
            for b in range(a + 1, size):
                value = value - schur[b][a] * answer[b]
            answer[a] = value / schur[a][a]
        weights = proj_sol
        for a in range(size):
            weights = jnp.where(row_at == base + a, answer[a], weights - solved[a] * answer[a])

        def combine(at, carry):
            span = pl.ds(pl.multiple_of(at * LANES, LANES), LANES)
            cur_x[:, span] = (
                est_x[:, span]
                - over_rows(hist_w[:, span] * weights[0:hist, :])
                - over_rows(new_w[:, span] * weights[base:rows, :])
            )
            return carry

        lax.fori_loop(0, full // LANES, combine, 0, unroll=2)
        if iteration + 1 < ITERS:
            cur_x[...] = jnp.where(outside, 0.0, cur_x[...])
            begin(iteration + 1)
    next_ref[...] = cur_x[:, LANES : LANES + width]
    last_ref[...] = old_res[...]


def shards(n_iface, n_dom, *args):
    width = args[0].shape[0]
    hist = args[5].shape[0]
    base = -(-hist // 8) * 8
    rows = base + 8
    count = n_iface * n_dom
    pairs = (base // 8 + 1) // 2
    share = -(-pairs // n_dom)
    depth = next(d for d in (512, 256, 128) if width % d == 0)
    assert hist <= 112
    full = width + 2 * LANES
    vectors = [a.reshape(1, width) for a in args[:5]]
    any_spec = pl.BlockSpec(memory_space=pl.ANY)
    vmem_spec = pl.BlockSpec(memory_space=pltpu.VMEM)
    outs = pl.pallas_call(
        functools.partial(kernel, (n_iface, n_dom, hist, base, rows, width, share, depth)),
        out_shape=[pltpu.VMEM((1, width), F32)] * 2,
        in_specs=[any_spec] * 7,
        out_specs=[vmem_spec] * 2,
        scratch_shapes=[
            pltpu.VMEM((1, full), F32),
            pltpu.VMEM((1, full), F32),
            pltpu.VMEM((1, full), F32),
            pltpu.VMEM((1, full), F32),
            pltpu.VMEM((1, width), F32),
            pltpu.VMEM((hist, width), F32),
            pltpu.VMEM((hist, full), F32),
            pltpu.VMEM((8, width), F32),
            pltpu.VMEM((8, full), F32),
            pltpu.VMEM((ITERS, 2, LANES), F32),
            pltpu.VMEM((LANES, LANES), F32),
            pltpu.VMEM((n_dom, 8 * share, LANES), F32),
            pltpu.VMEM((n_dom, 8 * share, LANES), F32),
            pltpu.VMEM((n_iface, 8 * share, LANES), F32),
            pltpu.VMEM((n_dom, 8 * share, LANES), F32),
            pltpu.VMEM((ITERS, count, 2, LANES), F32),
            pltpu.SemaphoreType.DMA((width // depth,)),
            pltpu.SemaphoreType.DMA((6,)),
            pltpu.SemaphoreType.DMA((2, 4, 2)),
            pltpu.SemaphoreType.DMA((2, 1, 2)),
            pltpu.SemaphoreType.DMA((2,)),
            pltpu.SemaphoreType.DMA((2,)),
            pltpu.SemaphoreType.DMA((2,)),
            pltpu.SemaphoreType.DMA((ITERS, 2)),
        ],
        compiler_params=pltpu.CompilerParams(collective_id=0, has_side_effects=True),
        name="coupling",
    )(*vectors, args[5], args[6])

    def finish(a, b, c, d, sems):
        copies = [pltpu.make_async_copy(a, c, sems.at[0]), pltpu.make_async_copy(b, d, sems.at[1])]
        for copy in copies:
            copy.start()
        for copy in copies:
            copy.wait()

    outs = pl.pallas_call(
        finish,
        out_shape=[jax.ShapeDtypeStruct((1, width), F32)] * 2,
        in_specs=[vmem_spec] * 2,
        out_specs=[any_spec] * 2,
        scratch_shapes=[pltpu.SemaphoreType.DMA((2,))],
        name="finish",
    )(*[pltpu.with_memory_space_constraint(o, pltpu.VMEM) for o in outs])
    return outs[0].reshape(width), outs[1].reshape(width)


def solution(mesh):
    one = P(AXES)
    return jax.shard_map(
        functools.partial(shards, mesh.shape["iface"], mesh.shape["dom"]),
        mesh=mesh,
        in_specs=(one,) * 5 + (P(None, AXES),) * 2,
        out_specs=(one, one),
        check_vma=False,
    )
```

```python
import functools
import jax
import jax.numpy as jnp
from jax import lax
from jax.experimental import pallas as pl
from jax.experimental.pallas import tpu as pltpu
from jax.sharding import PartitionSpec as P

ITERS = 3
coupling = 0.25
LANES = 128
AXES = ("iface", "dom")
F32 = jnp.float32


def invert(matrix, rows):
    lane8 = lax.broadcasted_iota(jnp.int32, (8, LANES), 1)
    sub8 = lax.broadcasted_iota(jnp.int32, (8, LANES), 0)
    blocks = [matrix[8 * at : 8 * at + 8, :] for at in range(rows // 8)]
    for step in range(rows // 8):
        first = 8 * step
        inside = (lane8 >= first) & (lane8 < first + 8)
        unit = (lane8 - first == sub8).astype(F32)
        pivots = blocks[step]
        columns = [jnp.broadcast_to(pivots[:, first + at : first + at + 1], (8, LANES)) for at in range(8)]
        panel = jnp.where(inside, unit, pivots)
        for at in range(8):
            inverse = 1.0 / columns[at][at : at + 1, :]
            own = sub8 == at
            factor = columns[at]
            row = panel[at : at + 1, :] * inverse
            panel = jnp.where(own, row, panel - factor * row)
            for later in range(at + 1, 8):
                row = columns[later][at : at + 1, :] * inverse
                columns[later] = jnp.where(own, row, columns[later] - factor * row)
        for other in range(rows // 8):
            if other != step:
                block = blocks[other]
                total = jnp.where(inside, 0.0, block)
                for at in range(8):
                    column = jnp.broadcast_to(block[:, first + at : first + at + 1], (8, LANES))
                    total = total - column * panel[at : at + 1, :]
                blocks[other] = total
        blocks[step] = panel
    return jnp.concatenate(blocks, axis=0)


def kernel(
    sizes,
    interface,
    previous_residual,
    previous_estimate,
    forcing,
    stiffness,
    history_residual,
    history_estimate,
    next_ref,
    last_ref,
    cur_x,
    est_x,
    force_x,
    stiff_x,
    old_res,
    hist_v,
    hist_w,
    new_v,
    new_w,
    dots_in,
    square,
    part_out,
    part_in,
    mid_in,
    gathered,
    row_in,
    piece_sem,
    load_sem,
    halo_sem,
    wide_sem,
    part_sem,
    mid_sem,
    gather_sem,
    row_sem,
):
    n_iface, n_dom, hist, base, rows, width, share, depth = sizes
    count = n_iface * n_dom
    at_iface, at_dom = lax.axis_index("iface"), lax.axis_index("dom")
    me = at_iface * n_dom + at_dom
    last = count - 1
    full = width + 2 * LANES
    ifaces = [lax.rem(at_iface + step, n_iface) for step in range(n_iface)]
    doms = [lax.rem(at_dom + step, n_dom) for step in range(n_dom)]
    everyone = [(a, b) for a in ifaces for b in doms][1:]

    def place(index):
        return (index // n_dom, lax.rem(index, n_dom))

    barrier = pltpu.get_barrier_semaphore()
    for device in everyone:
        pl.semaphore_signal(barrier, inc=1, device_id=device, device_id_type=pl.DeviceIdType.MESH)

    own = pl.ds(LANES, width)

    def piece(at):
        span = pl.ds(pl.multiple_of(at * depth, depth), depth)
        return pltpu.make_async_copy(history_residual.at[:, span], hist_v.at[:, span], piece_sem.at[at])

    for at in range(width // depth):
        piece(at).start()
    small = []
    for at, (source, target) in enumerate(
        [
            (interface, cur_x.at[:, own]),
            (previous_estimate, est_x.at[:, own]),
            (forcing, force_x.at[:, own]),
            (stiffness, stiff_x.at[:, own]),
            (previous_residual, old_res),
        ]
    ):
        copy = pltpu.make_async_copy(source, target, load_sem.at[1 + at])
        copy.start()
        small.append(copy)
    load_w = pltpu.make_async_copy(history_estimate, hist_w.at[:, own], load_sem.at[0])
    new_v[...] = jnp.zeros(new_v.shape, F32)
    new_w[...] = jnp.zeros(new_w.shape, F32)

    def add_gram(at, total):
        piece(at).wait()
        block = hist_v[:, pl.ds(pl.multiple_of(at * depth, depth), depth)]
        one = block.astype(jnp.bfloat16)
        rest = block - one.astype(F32)
        two = rest.astype(jnp.bfloat16)
        three = (rest - two.astype(F32)).astype(jnp.bfloat16)
        main = jnp.concatenate([one, two], axis=1)
        side = jnp.concatenate([two, three], axis=1), jnp.concatenate([one, one], axis=1)
        dims = (((1,), (1,)), ((), ()))
        return (
            total[0] + lax.dot_general(main, main, dims, preferred_element_type=F32),
            total[1] + lax.dot_general(*side, dims, preferred_element_type=F32),
        )

    empty = jnp.zeros((hist, hist), F32)
    main, side = lax.fori_loop(0, width // depth, add_gram, (empty, empty))
    load_w.start()
    square[...] = jnp.zeros(square.shape, F32)
    square[0:hist, 0:hist] = side
    mirrored = square[...].T
    square[0:hist, 0:hist] = main + side
    square[...] = square[...] + mirrored
    lane8 = lax.broadcasted_iota(jnp.int32, (8, LANES), 1)
    blocks = (base // 8 + 1) // 2 * 2
    pairs = blocks // 2

    def natural(block):
        return (lane8 >= 8 * block) & (lane8 < 8 * blocks)

    for pair in range(n_dom * share):
        where = (pair // share, pl.ds(8 * (pair % share), 8), slice(None))
        if pair < pairs:
            other = blocks - 1 - pair
            moved = pltpu.roll(square[8 * other : 8 * other + 8, :], 8 * pair + 8, 1)
            part_out[where] = jnp.where(natural(pair), square[8 * pair : 8 * pair + 8, :], moved)
        else:
            part_out[where] = jnp.zeros((8, LANES), F32)
    part_in[at_dom] = part_out[at_dom]
    for copy in small:
        copy.wait()
    pl.semaphore_wait(barrier, last)

    right = place(lax.rem(me + 1, count))
    left = place(lax.rem(me + last, count))

    def edges(refs, sems):
        copies = []
        for at, ref in enumerate(refs):
            for side, (source, target, device) in enumerate([(width, 0, right), (LANES, width + LANES, left)]):
                copies.append(
                    pltpu.make_async_remote_copy(
                        src_ref=ref.at[:, pl.ds(source, LANES)],
                        dst_ref=ref.at[:, pl.ds(target, LANES)],
                        send_sem=sems.at[0, at, side],
                        recv_sem=sems.at[1, at, side],
                        device_id=device,
                        device_id_type=pl.DeviceIdType.MESH,
                    )
                )
        return copies[0::2], copies[1::2]

    def edges_start(copies):
        for side, some in enumerate([me < last, me > 0]):

            @pl.when(some)
            def _():
                for copy in copies[side]:
                    copy.start()

    def edges_wait(copies):
        for side, (sent, received) in enumerate([(me < last, me > 0), (me > 0, me < last)]):

            @pl.when(sent)
            def _():
                for copy in copies[side]:
                    copy.wait_send()

            @pl.when(received)
            def _():
                for copy in copies[side]:
                    copy.wait_recv()

    def send(source, target, sems, device):
        pltpu.make_async_remote_copy(
            src_ref=source,
            dst_ref=target,
            send_sem=sems.at[0],
            recv_sem=sems.at[1],
            device_id=device,
            device_id_type=pl.DeviceIdType.MESH,
        ).start()

    def arrive(target, many, sems):
        most = target.at[pl.ds(0, many)]
        pltpu.make_async_copy(most, most, sems.at[1]).wait()
        pltpu.make_async_copy(most, most, sems.at[0]).wait()

    for dom in doms[1:]:
        send(part_out.at[dom], part_in.at[at_dom], part_sem, (at_iface, dom))
    halos = edges([cur_x, est_x, force_x, stiff_x], halo_sem)
    edges_start(halos)
    wide = edges([hist_w], wide_sem)

    lane = lax.broadcasted_iota(jnp.int32, (1, full), 1)
    outside = ((me == 0) & (lane < LANES)) | ((me == count - 1) & (lane >= LANES + width))
    eye = (
        lax.broadcasted_iota(jnp.int32, (rows, LANES), 0) == lax.broadcasted_iota(jnp.int32, (rows, LANES), 1)
    ).astype(F32)
    row_at = lax.broadcasted_iota(jnp.int32, (rows, LANES), 0)
    ones = jnp.ones((8, LANES), F32)

    def column_of(row):
        return jnp.broadcast_to(jnp.sum(eye * row, axis=1, keepdims=True), (rows, LANES))

    def over_rows(value):
        return jnp.sum(value, axis=0, keepdims=True)

    def begin(iteration):
        current = cur_x[...]
        before = pltpu.roll(current, 1, 1)
        after = pltpu.roll(current, full - 1, 1)
        estimate = force_x[...] + stiff_x[...] * jnp.tanh(current) + coupling * (before + after)
        residual = (estimate - current)[:, LANES : LANES + width]
        new_w[iteration : iteration + 1, :] = estimate - est_x[...]
        est_x[...] = estimate
        new_v[iteration : iteration + 1, :] = residual - old_res[...]
        old_res[...] = residual

        def add(at, totals):
            span = pl.ds(pl.multiple_of(at * LANES, LANES), LANES)
            block, extra = hist_v[:, span], new_v[:, span]
            res, new = old_res[:, span], new_v[iteration : iteration + 1, span]
            return (totals[0] + block * res, totals[1] + block * new, totals[2] + extra * res, totals[3] + extra * new)

        zero, few = jnp.zeros((hist, LANES), F32), jnp.zeros((8, LANES), F32)
        totals = lax.fori_loop(0, width // LANES, add, (zero, zero, few, few), unroll=4)
        dots_in[iteration] = jnp.zeros((2, LANES), F32)
        for which in range(4):
            sums = lax.dot_general(
                ones, totals[which], (((1,), (1,)), ((), ())), precision=lax.Precision.HIGHEST, preferred_element_type=F32
            )
            if which < 2:
                dots_in[iteration, which : which + 1, 0:hist] = sums[0:1, :]
            else:
                dots_in[iteration, which - 2 : which - 1, base : base + 8] = sums[0:1, :]
        row_in[iteration, me] = dots_in[iteration]
        for device in everyone:
            send(dots_in.at[iteration], row_in.at[iteration, me], row_sem.at[iteration], device)

    def sums_of(iteration):
        arrive(row_in.at[iteration], last, row_sem.at[iteration])
        return jnp.sum(row_in[iteration], axis=0)

    arrive(part_in, n_dom - 1, part_sem)
    mid_in[at_iface] = jnp.sum(part_in[...], axis=0)
    for iface in ifaces[1:]:
        send(mid_in.at[at_iface], mid_in.at[at_iface], mid_sem, (iface, at_dom))
    edges_wait(halos)
    cur_x[...] = jnp.where(outside, 0.0, cur_x[...])
    begin(0)
    load_w.wait()
    arrive(mid_in, n_iface - 1, mid_sem)
    gathered[at_dom] = jnp.sum(mid_in[...], axis=0)
    for dom in doms[1:]:
        send(gathered.at[at_dom], gathered.at[at_dom], gather_sem, (at_iface, dom))
    edges_start(wide)
    arrive(gathered, n_dom - 1, gather_sem)
    for pair in range(pairs):
        other = blocks - 1 - pair
        packed = gathered[pair // share, pl.ds(8 * (pair % share), 8), :]
        square[8 * pair : 8 * pair + 8, :] = jnp.where(natural(pair), packed, 0.0)
        moved = pltpu.roll(packed, LANES - 8 * pair - 8, 1)
        square[8 * other : 8 * other + 8, :] = jnp.where(natural(other), moved, 0.0)
    upper = square[...]
    lane_block = lax.broadcasted_iota(jnp.int32, (LANES, LANES), 1) // 8
    row_block = lax.broadcasted_iota(jnp.int32, (LANES, LANES), 0) // 8
    square[...] = jnp.where(lane_block >= row_block, upper, upper.T)
    kept = (row_at < hist) & (lax.broadcasted_iota(jnp.int32, (rows, LANES), 1) < hist)
    square[0:rows, :] = jnp.where(kept, square[0:rows, :], eye)
    square[0:base, :] = invert(square, base)
    square[0:rows, :] = jnp.where(kept, square[0:rows, :], 0.0)
    edges_wait(wide)

    solved, columns = [], []
    for iteration in range(ITERS):
        both = sums_of(iteration)
        proj, new = both[0:1, :], both[1:2, :]
        inverse = square[0:rows, :]
        proj_col, new_col = column_of(proj), column_of(new)
        proj_sol = jnp.broadcast_to(jnp.sum(inverse * proj, axis=1, keepdims=True), (rows, LANES))
        new_sol = jnp.broadcast_to(jnp.sum(inverse * new, axis=1, keepdims=True), (rows, LANES))
        solved.append(new_sol)
        columns.append(new_col)
        size = iteration + 1
        schur = [
            [columns[a][base + b : base + b + 1, :] - over_rows(columns[a] * solved[b]) for b in range(a + 1)]
            for a in range(size)
        ]
        right_side = [proj_col[base + a : base + a + 1, :] - over_rows(columns[a] * proj_sol) for a in range(size)]
        for a in range(size):
            for b in range(a + 1, size):
                factor = schur[b][a] / schur[a][a]
                right_side[b] = right_side[b] - factor * right_side[a]
                for c in range(a + 1, b + 1):
                    schur[b][c] = schur[b][c] - factor * schur[c][a]
        answer = [None] * size
        for a in reversed(range(size)):
            value = right_side[a]
            for b in range(a + 1, size):
                value = value - schur[b][a] * answer[b]
            answer[a] = value / schur[a][a]
        weights = proj_sol
        for a in range(size):
            weights = jnp.where(row_at == base + a, answer[a], weights - solved[a] * answer[a])

        def combine(at, carry):
            span = pl.ds(at * LANES if isinstance(at, int) else pl.multiple_of(at * LANES, LANES), LANES)
            total = new_w[:, span] * weights[base:rows, :]
            for first in range(0, hist, 8):
                some = min(8, hist - first)
                term = hist_w[first : first + some, span] * weights[first : first + some, :]
                if some < 8:
                    term = jnp.concatenate([term, jnp.zeros((8 - some, LANES), F32)], axis=0)
                total = total + term
            cur_x[:, span] = est_x[:, span] - over_rows(total)
            return carry

        lax.fori_loop(1, full // LANES - 1, combine, 0, unroll=4)
        if iteration + 1 < ITERS:
            combine(0, 0)
            combine(full // LANES - 1, 0)
            cur_x[...] = jnp.where(outside, 0.0, cur_x[...])
            begin(iteration + 1)
    next_ref[...] = cur_x[:, LANES : LANES + width]
    last_ref[...] = old_res[...]


def shards(n_iface, n_dom, *args):
    width = args[0].shape[0]
    hist = args[5].shape[0]
    base = -(-hist // 8) * 8
    rows = base + 8
    count = n_iface * n_dom
    pairs = (base // 8 + 1) // 2
    share = -(-pairs // n_dom)
    depth = next(d for d in (512, 256, 128) if width % d == 0)
    assert hist <= 112
    full = width + 2 * LANES
    vectors = [a.reshape(1, width) for a in args[:5]]
    any_spec = pl.BlockSpec(memory_space=pl.ANY)
    vmem_spec = pl.BlockSpec(memory_space=pltpu.VMEM)
    outs = pl.pallas_call(
        functools.partial(kernel, (n_iface, n_dom, hist, base, rows, width, share, depth)),
        out_shape=[pltpu.VMEM((1, width), F32)] * 2,
        in_specs=[any_spec] * 7,
        out_specs=[vmem_spec] * 2,
        scratch_shapes=[
            pltpu.VMEM((1, full), F32),
            pltpu.VMEM((1, full), F32),
            pltpu.VMEM((1, full), F32),
            pltpu.VMEM((1, full), F32),
            pltpu.VMEM((1, width), F32),
            pltpu.VMEM((hist, width), F32),
            pltpu.VMEM((hist, full), F32),
            pltpu.VMEM((8, width), F32),
            pltpu.VMEM((8, full), F32),
            pltpu.VMEM((ITERS, 2, LANES), F32),
            pltpu.VMEM((LANES, LANES), F32),
            pltpu.VMEM((n_dom, 8 * share, LANES), F32),
            pltpu.VMEM((n_dom, 8 * share, LANES), F32),
            pltpu.VMEM((n_iface, 8 * share, LANES), F32),
            pltpu.VMEM((n_dom, 8 * share, LANES), F32),
            pltpu.VMEM((ITERS, count, 2, LANES), F32),
            pltpu.SemaphoreType.DMA((width // depth,)),
            pltpu.SemaphoreType.DMA((6,)),
            pltpu.SemaphoreType.DMA((2, 4, 2)),
            pltpu.SemaphoreType.DMA((2, 1, 2)),
            pltpu.SemaphoreType.DMA((2,)),
            pltpu.SemaphoreType.DMA((2,)),
            pltpu.SemaphoreType.DMA((2,)),
            pltpu.SemaphoreType.DMA((ITERS, 2)),
        ],
        compiler_params=pltpu.CompilerParams(collective_id=0, has_side_effects=True),
        name="coupling",
    )(*vectors, args[5], args[6])

    def finish(a, b, c, d, sems):
        copies = [pltpu.make_async_copy(a, c, sems.at[0]), pltpu.make_async_copy(b, d, sems.at[1])]
        for copy in copies:
            copy.start()
        for copy in copies:
            copy.wait()

    outs = pl.pallas_call(
        finish,
        out_shape=[jax.ShapeDtypeStruct((1, width), F32)] * 2,
        in_specs=[vmem_spec] * 2,
        out_specs=[any_spec] * 2,
        scratch_shapes=[pltpu.SemaphoreType.DMA((2,))],
        name="finish",
    )(*[pltpu.with_memory_space_constraint(o, pltpu.VMEM) for o in outs])
    return outs[0].reshape(width), outs[1].reshape(width)


def solution(mesh):
    one = P(AXES)
    return jax.shard_map(
        functools.partial(shards, mesh.shape["iface"], mesh.shape["dom"]),
        mesh=mesh,
        in_specs=(one,) * 5 + (P(None, AXES),) * 2,
        out_specs=(one, one),
        check_vma=False,
    )
```

```python
import functools
import jax
import jax.numpy as jnp
from jax import lax
from jax.experimental import pallas as pl
from jax.experimental.pallas import tpu as pltpu
from jax.sharding import PartitionSpec as P

ITERS = 3
coupling = 0.25
LANES = 128
AXES = ("iface", "dom")
F32 = jnp.float32


def invert(matrix, rows):
    lane8 = lax.broadcasted_iota(jnp.int32, (8, LANES), 1)
    sub8 = lax.broadcasted_iota(jnp.int32, (8, LANES), 0)
    blocks = [matrix[8 * at : 8 * at + 8, :] for at in range(rows // 8)]
    for step in range(rows // 8):
        first = 8 * step
        inside = (lane8 >= first) & (lane8 < first + 8)
        unit = (lane8 - first == sub8).astype(F32)
        pivots = blocks[step]
        columns = [jnp.broadcast_to(pivots[:, first + at : first + at + 1], (8, LANES)) for at in range(8)]
        panel = jnp.where(inside, unit, pivots)
        for at in range(8):
            inverse = 1.0 / columns[at][at : at + 1, :]
            own = sub8 == at
            factor = columns[at]
            row = panel[at : at + 1, :] * inverse
            panel = jnp.where(own, row, panel - factor * row)
            for later in range(at + 1, 8):
                row = columns[later][at : at + 1, :] * inverse
                columns[later] = jnp.where(own, row, columns[later] - factor * row)
        for other in range(rows // 8):
            if other != step:
                block = blocks[other]
                total = jnp.where(inside, 0.0, block)
                for at in range(8):
                    column = jnp.broadcast_to(block[:, first + at : first + at + 1], (8, LANES))
                    total = total - column * panel[at : at + 1, :]
                blocks[other] = total
        blocks[step] = panel
    return jnp.concatenate(blocks, axis=0)


def kernel(
    sizes,
    interface,
    previous_residual,
    previous_estimate,
    forcing,
    stiffness,
    history_residual,
    history_estimate,
    next_ref,
    last_ref,
    cur_x,
    est_x,
    force_x,
    stiff_x,
    old_res,
    hist_v,
    hist_w,
    new_v,
    new_w,
    dots_in,
    square,
    part_out,
    part_in,
    mid_in,
    gathered,
    row_in,
    piece_sem,
    load_sem,
    halo_sem,
    wide_sem,
    part_sem,
    mid_sem,
    gather_sem,
    row_sem,
):
    n_iface, n_dom, hist, base, rows, width, share, depth = sizes
    count = n_iface * n_dom
    at_iface, at_dom = lax.axis_index("iface"), lax.axis_index("dom")
    me = at_iface * n_dom + at_dom
    last = count - 1
    full = width + 2 * LANES
    ifaces = [lax.rem(at_iface + step, n_iface) for step in range(n_iface)]
    doms = [lax.rem(at_dom + step, n_dom) for step in range(n_dom)]
    everyone = [(a, b) for a in ifaces for b in doms][1:]

    def place(index):
        return (index // n_dom, lax.rem(index, n_dom))

    barrier = pltpu.get_barrier_semaphore()

    def greet(device):
        pl.semaphore_signal(barrier, inc=1, device_id=device, device_id_type=pl.DeviceIdType.MESH)

    for iface in ifaces[1:]:
        greet((iface, at_dom))
    right = place(lax.rem(me + 1, count))
    left = place(lax.rem(me + last, count))
    greet(right)
    greet(left)
    for dom in doms[1:]:
        greet((at_iface, dom))

    own = pl.ds(LANES, width)

    def piece(at):
        span = pl.ds(pl.multiple_of(at * depth, depth), depth)
        return pltpu.make_async_copy(history_residual.at[:, span], hist_v.at[:, span], piece_sem.at[at])

    for at in range(width // depth):
        piece(at).start()
    small = []
    for at, (source, target) in enumerate(
        [
            (interface, cur_x.at[:, own]),
            (previous_estimate, est_x.at[:, own]),
            (forcing, force_x.at[:, own]),
            (stiffness, stiff_x.at[:, own]),
            (previous_residual, old_res),
        ]
    ):
        copy = pltpu.make_async_copy(source, target, load_sem.at[1 + at])
        copy.start()
        small.append(copy)
    load_w = pltpu.make_async_copy(history_estimate, hist_w.at[:, own], load_sem.at[0])
    new_v[...] = jnp.zeros(new_v.shape, F32)
    new_w[...] = jnp.zeros(new_w.shape, F32)

    def add_gram(at, total):
        piece(at).wait()
        block = hist_v[:, pl.ds(pl.multiple_of(at * depth, depth), depth)]
        one = block.astype(jnp.bfloat16)
        rest = block - one.astype(F32)
        two = rest.astype(jnp.bfloat16)
        three = (rest - two.astype(F32)).astype(jnp.bfloat16)
        main = jnp.concatenate([one, two], axis=1)
        side = jnp.concatenate([two, three], axis=1), jnp.concatenate([one, one], axis=1)
        dims = (((1,), (1,)), ((), ()))
        return (
            total[0] + lax.dot_general(main, main, dims, preferred_element_type=F32),
            total[1] + lax.dot_general(*side, dims, preferred_element_type=F32),
        )

    empty = jnp.zeros((hist, hist), F32)
    main, side = lax.fori_loop(0, width // depth, add_gram, (empty, empty))
    load_w.start()
    square[...] = jnp.zeros(square.shape, F32)
    square[0:hist, 0:hist] = side
    mirrored = square[...].T
    square[0:hist, 0:hist] = main + side
    square[...] = square[...] + mirrored
    lane8 = lax.broadcasted_iota(jnp.int32, (8, LANES), 1)
    blocks = (base // 8 + 1) // 2 * 2
    pairs = blocks // 2

    def natural(block):
        return (lane8 >= 8 * block) & (lane8 < 8 * blocks)

    for pair in range(n_dom * share):
        where = (pair // share, pl.ds(8 * (pair % share), 8), slice(None))
        if pair < pairs:
            other = blocks - 1 - pair
            moved = pltpu.roll(square[8 * other : 8 * other + 8, :], 8 * pair + 8, 1)
            part_out[where] = jnp.where(natural(pair), square[8 * pair : 8 * pair + 8, :], moved)
        else:
            part_out[where] = jnp.zeros((8, LANES), F32)
    part_in[at_dom] = part_out[at_dom]
    for copy in small:
        copy.wait()
    pl.semaphore_wait(barrier, n_iface + n_dom)

    def edges(refs, sems):
        copies = []
        for at, ref in enumerate(refs):
            for side, (source, target, device) in enumerate([(width, 0, right), (LANES, width + LANES, left)]):
                copies.append(
                    pltpu.make_async_remote_copy(
                        src_ref=ref.at[:, pl.ds(source, LANES)],
                        dst_ref=ref.at[:, pl.ds(target, LANES)],
                        send_sem=sems.at[0, at, side],
                        recv_sem=sems.at[1, at, side],
                        device_id=device,
                        device_id_type=pl.DeviceIdType.MESH,
                    )
                )
        return copies[0::2], copies[1::2]

    def edges_start(copies):
        for side, some in enumerate([me < last, me > 0]):

            @pl.when(some)
            def _():
                for copy in copies[side]:
                    copy.start()

    def edges_wait(copies):
        for side, (sent, received) in enumerate([(me < last, me > 0), (me > 0, me < last)]):

            @pl.when(sent)
            def _():
                for copy in copies[side]:
                    copy.wait_send()

            @pl.when(received)
            def _():
                for copy in copies[side]:
                    copy.wait_recv()

    def send(source, target, sems, device):
        pltpu.make_async_remote_copy(
            src_ref=source,
            dst_ref=target,
            send_sem=sems.at[0],
            recv_sem=sems.at[1],
            device_id=device,
            device_id_type=pl.DeviceIdType.MESH,
        ).start()

    def arrive(target, many, sems):
        most = target.at[pl.ds(0, many)]
        pltpu.make_async_copy(most, most, sems.at[1]).wait()
        pltpu.make_async_copy(most, most, sems.at[0]).wait()

    for dom in doms[1:]:
        send(part_out.at[dom], part_in.at[at_dom], part_sem, (at_iface, dom))
    halos = edges([cur_x, est_x, force_x, stiff_x], halo_sem)
    edges_start(halos)
    wide = edges([hist_w], wide_sem)

    lane = lax.broadcasted_iota(jnp.int32, (1, full), 1)
    outside = ((me == 0) & (lane < LANES)) | ((me == count - 1) & (lane >= LANES + width))
    eye = (
        lax.broadcasted_iota(jnp.int32, (rows, LANES), 0) == lax.broadcasted_iota(jnp.int32, (rows, LANES), 1)
    ).astype(F32)
    row_at = lax.broadcasted_iota(jnp.int32, (rows, LANES), 0)
    ones = jnp.ones((8, LANES), F32)

    def column_of(row):
        return jnp.broadcast_to(jnp.sum(eye * row, axis=1, keepdims=True), (rows, LANES))

    def over_rows(value):
        return jnp.sum(value, axis=0, keepdims=True)

    def begin(iteration):
        current = cur_x[...]
        before = pltpu.roll(current, 1, 1)
        after = pltpu.roll(current, full - 1, 1)
        estimate = force_x[...] + stiff_x[...] * jnp.tanh(current) + coupling * (before + after)
        residual = (estimate - current)[:, LANES : LANES + width]
        new_w[iteration : iteration + 1, :] = estimate - est_x[...]
        est_x[...] = estimate
        new_v[iteration : iteration + 1, :] = residual - old_res[...]
        old_res[...] = residual

        def add(at, totals):
            span = pl.ds(pl.multiple_of(at * LANES, LANES), LANES)
            block, extra = hist_v[:, span], new_v[:, span]
            res, new = old_res[:, span], new_v[iteration : iteration + 1, span]
            return (totals[0] + block * res, totals[1] + block * new, totals[2] + extra * res, totals[3] + extra * new)

        zero, few = jnp.zeros((hist, LANES), F32), jnp.zeros((8, LANES), F32)
        totals = lax.fori_loop(0, width // LANES, add, (zero, zero, few, few), unroll=4)
        dots_in[iteration] = jnp.zeros((2, LANES), F32)
        for which in range(4):
            sums = lax.dot_general(
                ones, totals[which], (((1,), (1,)), ((), ())), precision=lax.Precision.HIGHEST, preferred_element_type=F32
            )
            if which < 2:
                dots_in[iteration, which : which + 1, 0:hist] = sums[0:1, :]
            else:
                dots_in[iteration, which - 2 : which - 1, base : base + 8] = sums[0:1, :]
        row_in[iteration, me] = dots_in[iteration]
        for device in everyone:
            send(dots_in.at[iteration], row_in.at[iteration, me], row_sem.at[iteration], device)

    def sums_of(iteration):
        arrive(row_in.at[iteration], last, row_sem.at[iteration])
        return jnp.sum(row_in[iteration], axis=0)

    arrive(part_in, n_dom - 1, part_sem)
    mid_in[at_iface] = jnp.sum(part_in[...], axis=0)
    for iface in ifaces[1:]:
        send(mid_in.at[at_iface], mid_in.at[at_iface], mid_sem, (iface, at_dom))
    edges_wait(halos)
    cur_x[...] = jnp.where(outside, 0.0, cur_x[...])
    begin(0)
    load_w.wait()
    arrive(mid_in, n_iface - 1, mid_sem)
    gathered[at_dom] = jnp.sum(mid_in[...], axis=0)
    for dom in doms[1:]:
        send(gathered.at[at_dom], gathered.at[at_dom], gather_sem, (at_iface, dom))
    edges_start(wide)
    arrive(gathered, n_dom - 1, gather_sem)
    for pair in range(pairs):
        other = blocks - 1 - pair
        packed = gathered[pair // share, pl.ds(8 * (pair % share), 8), :]
        square[8 * pair : 8 * pair + 8, :] = jnp.where(natural(pair), packed, 0.0)
        moved = pltpu.roll(packed, LANES - 8 * pair - 8, 1)
        square[8 * other : 8 * other + 8, :] = jnp.where(natural(other), moved, 0.0)
    upper = square[...]
    lane_block = lax.broadcasted_iota(jnp.int32, (LANES, LANES), 1) // 8
    row_block = lax.broadcasted_iota(jnp.int32, (LANES, LANES), 0) // 8
    square[...] = jnp.where(lane_block >= row_block, upper, upper.T)
    kept = (row_at < hist) & (lax.broadcasted_iota(jnp.int32, (rows, LANES), 1) < hist)
    square[0:rows, :] = jnp.where(kept, square[0:rows, :], eye)
    square[0:base, :] = invert(square, base)
    square[0:rows, :] = jnp.where(kept, square[0:rows, :], 0.0)
    edges_wait(wide)

    solved, columns = [], []
    for iteration in range(ITERS):
        both = sums_of(iteration)
        proj, new = both[0:1, :], both[1:2, :]
        inverse = square[0:rows, :]
        proj_col, new_col = column_of(proj), column_of(new)
        proj_sol = jnp.broadcast_to(jnp.sum(inverse * proj, axis=1, keepdims=True), (rows, LANES))
        new_sol = jnp.broadcast_to(jnp.sum(inverse * new, axis=1, keepdims=True), (rows, LANES))
        solved.append(new_sol)
        columns.append(new_col)
        size = iteration + 1
        schur = [
            [columns[a][base + b : base + b + 1, :] - over_rows(columns[a] * solved[b]) for b in range(a + 1)]
            for a in range(size)
        ]
        right_side = [proj_col[base + a : base + a + 1, :] - over_rows(columns[a] * proj_sol) for a in range(size)]
        for a in range(size):
            for b in range(a + 1, size):
                factor = schur[b][a] / schur[a][a]
                right_side[b] = right_side[b] - factor * right_side[a]
                for c in range(a + 1, b + 1):
                    schur[b][c] = schur[b][c] - factor * schur[c][a]
        answer = [None] * size
        for a in reversed(range(size)):
            value = right_side[a]
            for b in range(a + 1, size):
                value = value - schur[b][a] * answer[b]
            answer[a] = value / schur[a][a]
        weights = proj_sol
        for a in range(size):
            weights = jnp.where(row_at == base + a, answer[a], weights - solved[a] * answer[a])

        def combine(at, carry):
            span = pl.ds(at * LANES if isinstance(at, int) else pl.multiple_of(at * LANES, LANES), LANES)
            total = new_w[:, span] * weights[base:rows, :]
            for first in range(0, hist, 8):
                some = min(8, hist - first)
                term = hist_w[first : first + some, span] * weights[first : first + some, :]
                if some < 8:
                    term = jnp.concatenate([term, jnp.zeros((8 - some, LANES), F32)], axis=0)
                total = total + term
            cur_x[:, span] = est_x[:, span] - over_rows(total)
            return carry

        lax.fori_loop(1, full // LANES - 1, combine, 0, unroll=4)
        if iteration + 1 < ITERS:
            combine(0, 0)
            combine(full // LANES - 1, 0)
            cur_x[...] = jnp.where(outside, 0.0, cur_x[...])
            begin(iteration + 1)
    next_ref[...] = cur_x[:, LANES : LANES + width]
    last_ref[...] = old_res[...]


def shards(n_iface, n_dom, *args):
    width = args[0].shape[0]
    hist = args[5].shape[0]
    base = -(-hist // 8) * 8
    rows = base + 8
    count = n_iface * n_dom
    pairs = (base // 8 + 1) // 2
    share = -(-pairs // n_dom)
    depth = next(d for d in (512, 256, 128) if width % d == 0)
    assert hist <= 112
    full = width + 2 * LANES
    vectors = [a.reshape(1, width) for a in args[:5]]
    any_spec = pl.BlockSpec(memory_space=pl.ANY)
    vmem_spec = pl.BlockSpec(memory_space=pltpu.VMEM)
    outs = pl.pallas_call(
        functools.partial(kernel, (n_iface, n_dom, hist, base, rows, width, share, depth)),
        out_shape=[pltpu.VMEM((1, width), F32)] * 2,
        in_specs=[any_spec] * 7,
        out_specs=[vmem_spec] * 2,
        scratch_shapes=[
            pltpu.VMEM((1, full), F32),
            pltpu.VMEM((1, full), F32),
            pltpu.VMEM((1, full), F32),
            pltpu.VMEM((1, full), F32),
            pltpu.VMEM((1, width), F32),
            pltpu.VMEM((hist, width), F32),
            pltpu.VMEM((hist, full), F32),
            pltpu.VMEM((8, width), F32),
            pltpu.VMEM((8, full), F32),
            pltpu.VMEM((ITERS, 2, LANES), F32),
            pltpu.VMEM((LANES, LANES), F32),
            pltpu.VMEM((n_dom, 8 * share, LANES), F32),
            pltpu.VMEM((n_dom, 8 * share, LANES), F32),
            pltpu.VMEM((n_iface, 8 * share, LANES), F32),
            pltpu.VMEM((n_dom, 8 * share, LANES), F32),
            pltpu.VMEM((ITERS, count, 2, LANES), F32),
            pltpu.SemaphoreType.DMA((width // depth,)),
            pltpu.SemaphoreType.DMA((6,)),
            pltpu.SemaphoreType.DMA((2, 4, 2)),
            pltpu.SemaphoreType.DMA((2, 1, 2)),
            pltpu.SemaphoreType.DMA((2,)),
            pltpu.SemaphoreType.DMA((2,)),
            pltpu.SemaphoreType.DMA((2,)),
            pltpu.SemaphoreType.DMA((ITERS, 2)),
        ],
        compiler_params=pltpu.CompilerParams(collective_id=0, has_side_effects=True),
        name="coupling",
    )(*vectors, args[5], args[6])

    def finish(a, b, c, d, sems):
        copies = [pltpu.make_async_copy(a, c, sems.at[0]), pltpu.make_async_copy(b, d, sems.at[1])]
        for copy in copies:
            copy.start()
        for copy in copies:
            copy.wait()

    outs = pl.pallas_call(
        finish,
        out_shape=[jax.ShapeDtypeStruct((1, width), F32)] * 2,
        in_specs=[vmem_spec] * 2,
        out_specs=[any_spec] * 2,
        scratch_shapes=[pltpu.SemaphoreType.DMA((2,))],
        name="finish",
    )(*[pltpu.with_memory_space_constraint(o, pltpu.VMEM) for o in outs])
    return outs[0].reshape(width), outs[1].reshape(width)


def solution(mesh):
    one = P(AXES)
    return jax.shard_map(
        functools.partial(shards, mesh.shape["iface"], mesh.shape["dom"]),
        mesh=mesh,
        in_specs=(one,) * 5 + (P(None, AXES),) * 2,
        out_specs=(one, one),
        check_vma=False,
    )
```
